32 devices in a mesh: gx: 8 (over z, y), gy: 4 (over x, core).
Axes of the slice: x: 2, y: 2, z: 4, core: 2. Of those that a mesh axis runs over, the one named last changes fastest.
Arguments:
- velocity: float32 [3, 64, 256, 384], P(None, 'gx', 'gy')
- target_profile: float32 [2, 384], replicated, may hold values from 0.5 to 1.5
- disc_turbine: int32 [32, 4], P(('gx', 'gy')), may hold values from -1 to 99, as said below
- disc_start: int32 [3, 32, 4], P(None, ('gx', 'gy')), may hold values from 0 to 256, as said below
- disc_weight: float32 [32, 4, 16, 128], P(('gx', 'gy')), may hold values from 0.2 to 1
- turbine_owner: int32 [100], replicated, may hold values from 0 to 31, as said below
- mode_flag: int32 [100], replicated, may hold values from 0 to 2
- controller_state: float32 [32, 4], P(('gx', 'gy')), may hold values from -4 to 4
Outputs:
- advanced_velocity: float32 [3, 64, 256, 384], P(None, 'gx', 'gy')
- profiles: float32 [4, 384], replicated
- thrust_setpoint: float32 [100], replicated
- controller_next: float32 [32, 4], P(('gx', 'gy'))
The draws below stay inside these ranges and needn't reach their ends.
Inputs may be any that keep to these rules, and one draw needn't show every extreme that they name: `disc_turbine`: -1 marks an empty slot; every turbine number appears in at least one slot; some device has all 4 slots filled. `disc_start`: row 0 is a cell of the device's block along the first dimension, 0 to 7; row 1 the first of 16 cells along the second, 0 to 48; row 2 the first of 128 heights, 0 to 256. `turbine_owner`: no device owns more than 4 turbines, and some device owns exactly 4.
All inputs are finite; a program needn't handle non-finite values.
Results may differ from the reference program's by a relative error of at most 0.00013.
Values sent between devices are 32-bit elements; how exact they have to be, the bound alone decides.
A program may use at most 128 MiB of HBM per device.

```python
import math
import jax
import jax.numpy as jnp
from jax import lax

CX = 8
CY = 64
NZ = 384
STEPS = 4
NT = 100
SLOTS = 4
OWN = 4
TY = 16
TZ = 128
NX = 64
NY = 256
N_GX = 8
N_GY = 4


def draw_velocity(key, part):
    key_u, key_v, key_w = jax.random.split(key, 3)
    shape = (NX, NY, NZ)
    height = (jnp.arange(NZ, dtype=jnp.float32) + 0.5) / NZ
    mean_wind = 0.4 + 0.8 * jnp.log1p(40.0 * height) / jnp.log1p(40.0)
    along = (jnp.arange(NX, dtype=jnp.float32) + 0.5) / NX
    rough_u = jax.random.normal(key_u, shape, jnp.float32)
    rough_v = jax.random.normal(key_v, shape, jnp.float32)
    rough_w = jax.random.normal(key_w, shape, jnp.float32)
    amplitude = 0.1 * (1.0 + 2.0 * along)[:, None, None]
    smooth_part = jnp.zeros((1, NY, 1), jnp.float32)
    component_u = mean_wind[None, None, :] + smooth_part + amplitude * rough_u
    component_v = amplitude * rough_v
    component_w = 0.5 * amplitude * rough_w
    return jnp.stack([component_u, component_v, component_w]).astype(jnp.float32)


def draw_disc_turbine(key, part):
    devices = N_GX * N_GY
    total_slots = devices * SLOTS
    key_order, key_heavy = jax.random.split(jax.random.fold_in(key, 7))
    position = jax.random.permutation(key_order, total_slots).astype(jnp.int32)
    heavy_rank = jax.random.permutation(key_heavy, devices).astype(jnp.int32)
    heavy_device = heavy_rank < max(1, devices // 4)
    heavy_slot = jnp.repeat(heavy_device, SLOTS)
    live_slot = (position < NT) | heavy_slot
    return jnp.where(live_slot, position % NT, -1).astype(jnp.int32).reshape(devices, SLOTS)


def draw_disc_start(key, part):
    devices = N_GX * N_GY
    key_x, key_y, key_z = jax.random.split(jax.random.fold_in(key, 3), 3)
    shape = (devices, SLOTS)
    first_x = jax.random.randint(key_x, shape, 0, CX)
    first_y = jax.random.randint(key_y, shape, 0, CY - TY + 1)
    first_z = jax.random.randint(key_z, shape, 0, NZ - TZ + 1)
    return jnp.stack([first_x, first_y, first_z]).astype(jnp.int32)


def draw_turbine_owner(key, part):
    devices = N_GX * N_GY
    key_group, key_device = jax.random.split(jax.random.fold_in(key, 5))
    turbine_order = jax.random.permutation(key_group, NT).astype(jnp.int32)
    device_order = jax.random.permutation(key_device, devices).astype(jnp.int32)
    return device_order[turbine_order // OWN].astype(jnp.int32)


def set_ends(array, stream_key, least, top_value):
    longest = array.shape.index(max(array.shape))
    spots = []
    for shift in (0, 1):
        where = [jax.random.randint(jax.random.fold_in(stream_key, axis), (), 0, length) for axis, length in enumerate(array.shape)]
        where[longest] = (where[longest] + shift) % array.shape[longest]
        spots.append(tuple(where))
    return array.at[spots[0]].set(least).at[spots[1]].set(top_value)


def steps_of(rng, shape, pieces, low, high):
    level = 1.0
    for dim, parts in pieces:
        draws = jax.random.uniform(jax.random.fold_in(jax.random.fold_in(rng, 6), dim), (parts,), jnp.float32, low / len(pieces), high / len(pieces))
        level = level * jnp.repeat(jnp.exp(draws), shape[dim] // parts).reshape((-1,) + (1,) * (len(shape) - 1 - dim))
    return level


def bell_draw(stream_key, dims, deviation, bound, shards=(), kind=jnp.bfloat16):
    loudness = steps_of(stream_key, dims, shards, -0.22, 0.18) if shards else 1.0
    result = jax.random.normal(stream_key, dims, jnp.float32) * deviation * loudness
    return jnp.minimum(jnp.maximum(result, -bound), bound).astype(kind)


def setup_inputs(seed: int = 0) -> dict:
    keys = jax.random.split(jax.random.key(seed), 9)
    return {
        "velocity": draw_velocity(jax.random.fold_in(keys[8], 71), 0),
        "target_profile": jnp.clip(jax.random.uniform(keys[1], (2, NZ), jnp.float32, 0.5, 1.5), 0.5, 1.5),
        "disc_turbine": draw_disc_turbine(jax.random.fold_in(keys[8], 71), 0),
        "disc_start": draw_disc_start(jax.random.fold_in(keys[8], 71), 0),
        "disc_weight": jnp.clip(jnp.exp(math.log(1.0) - 1.609438 * jax.random.uniform(keys[4], (N_GX * N_GY, SLOTS, TY, TZ), jnp.float32) ** steps_of(keys[4], (N_GX * N_GY, SLOTS, TY, TZ), ((0, 32),), -0.2, 0.2)), 0.2, 1.0),
        "turbine_owner": draw_turbine_owner(jax.random.fold_in(keys[8], 71), 0),
        "mode_flag": set_ends(jax.random.randint(keys[6], (NT,), 0, 3), jax.random.fold_in(keys[6], 1), 0, 2).astype(jnp.int32),
        "controller_state": bell_draw(keys[7], (N_GX * N_GY, OWN), 1.0, 4.0, ((0, 32),), jnp.float32),
    }


VISCOSITY = 0.1
TIME_STEP = 0.2
RELAX_TIME = 2.0
CONTROL_STEP = 0.5
GAIN_PROPORTIONAL = 2.0
GAIN_INTEGRAL = 1.0
HIGHEST = lax.Precision.HIGHEST


def neighbours(field, direction, offset):
    if direction == 2:
        extent = field.shape[2]
        padded = jnp.pad(field, ((0, 0), (0, 0), (2, 2)))
        return padded[:, :, 2 + offset:2 + offset + extent]
    return jnp.roll(field, -offset, direction)


def derivative(field, direction):
    return (8.0 * (neighbours(field, direction, 1) - neighbours(field, direction, -1)) - (neighbours(field, direction, 2) - neighbours(field, direction, -2))) / 12.0


def tendency(velocity):
    results = []
    for component in range(3):
        field = velocity[component]
        laplacian = (neighbours(field, 0, 1) + neighbours(field, 0, -1)) + (neighbours(field, 1, 1) + neighbours(field, 1, -1)) + (neighbours(field, 2, 1) + neighbours(field, 2, -1)) - 6.0 * field
        advection = velocity[0] * derivative(field, 0) + velocity[1] * derivative(field, 1) + velocity[2] * derivative(field, 2)
        results.append(VISCOSITY * laplacian - advection)
    return jnp.stack(results)


def control_terms(mode_flag):
    rated_speed = jnp.where(mode_flag == 0, 0.7, jnp.where(mode_flag == 1, 0.9, 1.1)).astype(jnp.float32)
    bias_terms = jnp.where(mode_flag == 0, 1.0, jnp.where(mode_flag == 1, 0.0, -1.0)).astype(jnp.float32)
    return rated_speed, bias_terms


def owner_rank(turbine_owner):
    turbines = turbine_owner.shape[0]
    same_owner = turbine_owner[:, None] == turbine_owner[None, :]
    earlier = jnp.arange(turbines, dtype=jnp.int32)[None, :] < jnp.arange(turbines, dtype=jnp.int32)[:, None]
    return jnp.sum((same_owner & earlier).astype(jnp.int32), axis=1).astype(jnp.int32)


def reference(velocity, target_profile, disc_turbine, disc_start, disc_weight, turbine_owner, mode_flag, controller_state):
    devices = N_GX * N_GY
    total_slots = devices * SLOTS
    slot_turbine = disc_turbine.reshape(total_slots)
    device_index = jnp.repeat(jnp.arange(devices, dtype=jnp.int32), SLOTS)
    start_x = ((device_index // N_GY) * CX + disc_start[0].reshape(total_slots)).astype(jnp.int32)
    start_y = ((device_index % N_GY) * CY + disc_start[1].reshape(total_slots)).astype(jnp.int32)
    start_z = disc_start[2].reshape(total_slots).astype(jnp.int32)
    weights_flat = disc_weight.reshape(total_slots, TY, TZ)
    slot_onehot = (slot_turbine[:, None] == jnp.arange(NT, dtype=jnp.int32)[None, :]).astype(jnp.float32)
    disc_area = jnp.dot(jnp.sum(weights_flat, axis=(1, 2)), slot_onehot, precision=HIGHEST)
    owner_slot = owner_rank(turbine_owner)
    owner_column = (turbine_owner * OWN + owner_slot).astype(jnp.int32)
    state_flat = controller_state.reshape(devices * OWN)
    integral = state_flat[owner_column]
    rated_speed, bias_terms = control_terms(mode_flag)
    profiles = jnp.zeros((4, NZ), jnp.float32)
    thrust = jnp.zeros((NT,), jnp.float32)
    for turn_index in range(STEPS):
        streamwise = velocity[0]

        def disc_probe(slot_index):
            window_cells = lax.dynamic_slice(streamwise, (start_x[slot_index], start_y[slot_index], start_z[slot_index]), (1, TY, TZ))[0]
            return jnp.sum(weights_flat[slot_index] * window_cells)

        contribution = lax.map(disc_probe, jnp.arange(total_slots, dtype=jnp.int32))
        numerator = jnp.dot(contribution, slot_onehot, precision=HIGHEST)
        disc_speed = numerator / disc_area
        plane_sums = jnp.stack([jnp.sum(velocity[0], axis=(0, 1)), jnp.sum(velocity[1], axis=(0, 1)), jnp.sum(velocity[2], axis=(0, 1)), jnp.sum(velocity[0] * velocity[2], axis=(0, 1))])
        plane_means = plane_sums / (NX * NY)
        profiles = profiles + jnp.stack([plane_means[0], plane_means[1], plane_means[2], plane_means[3] - plane_means[0] * plane_means[2]])
        speed_error = disc_speed - rated_speed
        integral = integral + CONTROL_STEP * speed_error
        thrust = 0.1 + 0.9 * jax.nn.sigmoid(bias_terms - GAIN_PROPORTIONAL * speed_error - GAIN_INTEGRAL * integral)
        thrust_factor = 0.5 * thrust * disc_speed * jnp.abs(disc_speed)
        slot_factor = jnp.dot(slot_onehot, thrust_factor, precision=HIGHEST)

        def add_tile(slot_index, force_field):
            corner = (start_x[slot_index], start_y[slot_index], start_z[slot_index])
            previous = lax.dynamic_slice(force_field, corner, (1, TY, TZ))
            return lax.dynamic_update_slice(force_field, previous - slot_factor[slot_index] * weights_flat[slot_index][None], corner)

        force_field = lax.fori_loop(0, total_slots, add_tile, jnp.zeros((NX, NY, NZ), jnp.float32))
        nudging = (target_profile - plane_means[0:2]) / RELAX_TIME
        changes = tendency(velocity)
        velocity = jnp.stack([
            velocity[0] + TIME_STEP * (changes[0] + nudging[0][None, None, :] + force_field),
            velocity[1] + TIME_STEP * (changes[1] + nudging[1][None, None, :]),
            velocity[2] + TIME_STEP * changes[2]])
    controller_next = state_flat.at[owner_column].set(integral).reshape(devices, OWN)
    return velocity, profiles / STEPS, thrust, controller_next
```

```python
import functools

import jax
import jax.numpy as jnp
from jax import lax
from jax.experimental import pallas as pl
from jax.experimental.pallas import tpu as pltpu
from jax.sharding import PartitionSpec as P

STEPS = 4

VISCOSITY = 0.1
TIME_STEP = 0.2
RELAX_TIME = 2.0
CONTROL_STEP = 0.5
GAIN_PROPORTIONAL = 2.0
GAIN_INTEGRAL = 1.0
HIGHEST = lax.Precision.HIGHEST
MESH = pl.DeviceIdType.MESH
PAD = 8
CHUNKS = 2


def kernel(
    n_gx,
    n_gy,
    vel_ref,
    target_ref,
    turbine_ref,
    start_ref,
    weight_ref,
    owner_ref,
    mode_ref,
    state_ref,
    out_ref,
    prof_ref,
    thrust_ref,
    next_ref,
    buf,
    dense,
    acc,
    acc_disc,
    pay,
    gather_y,
    gather_x,
    send_x,
    recv_x,
    send_y,
    recv_y,
    load_sem,
    send_1,
    recv_1,
    send_2,
    recv_2,
    integral_ref,
    area_ref,
    factor_ref,
    mine_ref,
    nudge_ref,
):
    len_x, len_y, len_z = vel_ref.shape[1:]
    slots, tile_y, tile_z = weight_ref.shape[1:]
    owned = state_ref.shape[1]
    turbines = owner_ref.shape[1]
    gx = lax.axis_index("gx")
    gy = lax.axis_index("gy")
    right_x = (lax.rem(gx + 1, n_gx), gy)
    left_x = (lax.rem(gx + n_gx - 1, n_gx), gy)
    right_y = (gx, lax.rem(gy + 1, n_gy))
    left_y = (gx, lax.rem(gy + n_gy - 1, n_gy))
    rows = len_y // CHUNKS

    barrier = pltpu.get_barrier_semaphore()
    for d in range(1, n_gy):
        pl.semaphore_signal(barrier, inc=1, device_id=(gx, lax.rem(gy + d, n_gy)), device_id_type=MESH)
    for d in range(1, n_gx):
        pl.semaphore_signal(barrier, inc=1, device_id=(lax.rem(gx + d, n_gx), gy), device_id_type=MESH)

    load = pltpu.make_async_copy(
        vel_ref, buf.at[0, :, pl.ds(2, len_x), pl.ds(PAD, len_y), :], load_sem
    )
    load.start()
    pl.semaphore_wait(barrier, n_gx + n_gy - 2)

    def x_copy(parity, side, chunk, first):
        at = PAD + chunk * rows
        begin = len_x - 2 if side == 0 else 0
        if first:
            source = vel_ref.at[:, pl.ds(begin, 2), pl.ds(chunk * rows, rows), :]
        else:
            source = buf.at[parity, :, pl.ds(begin + 2, 2), pl.ds(at, rows), :]
        place = 0 if side == 0 else len_x + 2
        return pltpu.make_async_remote_copy(
            src_ref=source,
            dst_ref=buf.at[parity, :, pl.ds(place, 2), pl.ds(at, rows), :],
            send_sem=send_x.at[side, chunk],
            recv_sem=recv_x.at[parity, side, chunk],
            device_id=right_x if side == 0 else left_x,
            device_id_type=MESH,
        )

    def y_copy(parity, side, first):
        begin = len_y - PAD if side == 0 else 0
        if first:
            source = vel_ref.at[:, :, pl.ds(begin, PAD), :]
        else:
            source = buf.at[parity, :, pl.ds(2, len_x), pl.ds(PAD + begin, PAD), :]
        place = 0 if side == 0 else PAD + len_y
        return pltpu.make_async_remote_copy(
            src_ref=source,
            dst_ref=buf.at[parity, :, pl.ds(2, len_x), pl.ds(place, PAD), :],
            send_sem=send_y.at[side],
            recv_sem=recv_y.at[parity, side],
            device_id=right_y if side == 0 else left_y,
            device_id_type=MESH,
        )

    for side in range(2):
        y_copy(0, side, True).start()
    for chunk in range(CHUNKS):
        for side in range(2):
            x_copy(0, side, chunk, True).start()

    for s in range(slots):
        rows_hot = (
            lax.broadcasted_iota(jnp.int32, (len_y, tile_y), 0)
            - lax.broadcasted_iota(jnp.int32, (len_y, tile_y), 1)
            == start_ref[1, 0, s]
        ).astype(jnp.float32)
        cols_hot = (
            lax.broadcasted_iota(jnp.int32, (tile_z, len_z), 1)
            - lax.broadcasted_iota(jnp.int32, (tile_z, len_z), 0)
            == start_ref[2, 0, s]
        ).astype(jnp.float32)
        tall = jnp.dot(rows_hot, weight_ref[0, s], precision=HIGHEST, preferred_element_type=jnp.float32)
        dense[s] = jnp.dot(tall, cols_hot, precision=HIGHEST, preferred_element_type=jnp.float32)

    lane_t = lax.broadcasted_iota(jnp.int32, (1, turbines), 1)

    def hot(s):
        return (lane_t == turbine_ref[0, s]).astype(jnp.float32)

    owner = owner_ref[...]
    me = gx * n_gy + gy
    pair_row = lax.broadcasted_iota(jnp.int32, (turbines, turbines), 0)
    pair_col = lax.broadcasted_iota(jnp.int32, (turbines, turbines), 1)
    owner_f = owner.astype(jnp.float32)
    owner_column = jnp.sum(jnp.where(pair_row == pair_col, owner_f, 0.0), axis=1, keepdims=True)
    rank = jnp.sum(
        jnp.where((owner_column == owner_f) & (pair_row < pair_col), 1.0, 0.0), axis=0, keepdims=True
    )
    is_me = jnp.where(owner == me, 1.0, 0.0)
    mine_integral = jnp.zeros((1, turbines), jnp.float32)
    area = jnp.zeros((1, turbines), jnp.float32)
    for r in range(owned):
        mine_r = jnp.where(rank == float(r), is_me, 0.0)
        mine_ref[r : r + 1, :] = mine_r
        mine_integral = mine_integral + mine_r * state_ref[0, r]
    for s in range(slots):
        area = area + jnp.sum(weight_ref[0, s]) * hot(s)
    pay[...] = jnp.zeros_like(pay)
    pay[0, 5:6, 0:turbines] = area
    pay[0, 6:7, 0:turbines] = mine_integral

    mode = mode_ref[...]
    rated = jnp.where(mode == 0, 0.7, jnp.where(mode == 1, 0.9, 1.1)).astype(jnp.float32)
    bias = jnp.where(mode == 0, 1.0, jnp.where(mode == 1, 0.0, -1.0)).astype(jnp.float32)
    prof_ref[...] = jnp.zeros_like(prof_ref)

    lane = lax.broadcasted_iota(jnp.int32, (8, len_z), 1)
    keep_m1 = lane >= 1
    keep_m2 = lane >= 2
    keep_p1 = lane < len_z - 1
    keep_p2 = lane < len_z - 2

    def fold(value):
        total = value[:, 0:128]
        for z in range(128, len_z, 128):
            total = total + value[:, z : z + 128]
        return total

    def tally(x, values):
        sums = None
        discs = [None] * slots
        for group, u, v, w in values:
            terms = [u, v, w, u * w]
            sums = terms if sums is None else [a + b for a, b in zip(sums, terms)]
            for s in range(slots):
                part = dense[s, group : group + 8, :] * u
                discs[s] = part if discs[s] is None else discs[s] + part
        for c in range(4):
            acc[c] += sums[c]
        for s in range(slots):
            here = jnp.where(start_ref[0, 0, s] == x, 1.0, 0.0)
            acc_disc[s] += fold(discs[s]) * here

    def reset():
        acc[...] = jnp.zeros_like(acc)
        acc_disc[...] = jnp.zeros_like(acc_disc)

    def first_plane(x, carry):
        tally(
            x,
            [
                (g, *[buf[0, c, x + 2, PAD + g : PAD + g + 8, :] for c in range(3)])
                for g in range(0, len_y, 8)
            ],
        )
        return carry

    def update(parity, x, group):
        at = PAD + group

        def cells(c, dx, dy):
            return buf[parity, c, x + 2 + dx, at + dy : at + dy + 8, :]

        centre = [cells(c, 0, 0) for c in range(3)]
        scaled = [f * (TIME_STEP / 12.0) for f in centre]
        fresh = []
        for c in range(3):
            f = centre[c]
            xp, xm = cells(c, 1, 0), cells(c, -1, 0)
            yp, ym = cells(c, 0, 1), cells(c, 0, -1)
            zp = jnp.where(keep_p1, pltpu.roll(f, len_z - 1, 1), 0.0)
            zm = jnp.where(keep_m1, pltpu.roll(f, 1, 1), 0.0)
            zp2 = jnp.where(keep_p2, pltpu.roll(f, len_z - 2, 1), 0.0)
            zm2 = jnp.where(keep_m2, pltpu.roll(f, 2, 1), 0.0)
            grad_x = 8.0 * (xp - xm) - (cells(c, 2, 0) - cells(c, -2, 0))
            grad_y = 8.0 * (yp - ym) - (cells(c, 0, 2) - cells(c, 0, -2))
            grad_z = 8.0 * (zp - zm) - (zp2 - zm2)
            around = (xp + xm) + (yp + ym) + (zp + zm)
            advection = scaled[0] * grad_x + scaled[1] * grad_y + scaled[2] * grad_z
            fresh.append(
                (1.0 - 6.0 * TIME_STEP * VISCOSITY) * f + (TIME_STEP * VISCOSITY) * around - advection
            )
        push = nudge_ref[0]
        for s in range(slots):
            gain = jnp.where(start_ref[0, 0, s] == x, factor_ref[s], 0.0)
            push = push + gain * dense[s, group : group + 8, :]
        fresh[0] = fresh[0] + push
        fresh[1] = fresh[1] + nudge_ref[1]
        for c in range(3):
            buf[1 - parity, c, x + 2, at : at + 8, :] = fresh[c]
        return (group, *fresh)

    def sweep(parity, x, lower, upper):
        tally(x, [update(parity, x, g) for g in range(lower, upper, 8)])

    def reduce_all(parity):
        numerator = jnp.zeros((1, turbines), jnp.float32)
        for s in range(slots):
            numerator = numerator + jnp.sum(acc_disc[s]) * hot(s)
        for c in range(4):
            pay[0, c : c + 1, 0:len_z] = jnp.sum(acc[c], axis=0, keepdims=True)
        pay[0, 4:5, 0:turbines] = numerator
        copies = []
        for d in range(1, n_gy):
            copies.append(
                pltpu.make_async_remote_copy(
                    src_ref=pay.at[0],
                    dst_ref=gather_y.at[parity, gy],
                    send_sem=send_1.at[d],
                    recv_sem=recv_1.at[parity, gy],
                    device_id=(gx, lax.rem(gy + d, n_gy)),
                    device_id_type=MESH,
                )
            )
            copies[-1].start()
        gather_y[parity, gy] = pay[0]
        for d in range(1, n_gy):
            sender = lax.rem(gy + d, n_gy)
            pltpu.make_async_remote_copy(
                src_ref=pay.at[0],
                dst_ref=gather_y.at[parity, sender],
                send_sem=send_1.at[d],
                recv_sem=recv_1.at[parity, sender],
                device_id=(gx, sender),
                device_id_type=MESH,
            ).wait_recv()
        total = gather_y[parity, 0]
        for d in range(1, n_gy):
            total = total + gather_y[parity, d]
        pay[1] = total
        for d in range(1, n_gx):
            copies.append(
                pltpu.make_async_remote_copy(
                    src_ref=pay.at[1],
                    dst_ref=gather_x.at[parity, gx],
                    send_sem=send_2.at[d],
                    recv_sem=recv_2.at[parity, gx],
                    device_id=(lax.rem(gx + d, n_gx), gy),
                    device_id_type=MESH,
                )
            )
            copies[-1].start()
        gather_x[parity, gx] = total
        for d in range(1, n_gx):
            sender = lax.rem(gx + d, n_gx)
            pltpu.make_async_remote_copy(
                src_ref=pay.at[1],
                dst_ref=gather_x.at[parity, sender],
                send_sem=send_2.at[d],
                recv_sem=recv_2.at[parity, sender],
                device_id=(sender, gy),
                device_id_type=MESH,
            ).wait_recv()
        for copy in copies:
            copy.wait_send()
        total = gather_x[parity, 0]
        for d in range(1, n_gx):
            total = total + gather_x[parity, d]
        return total

    cells_total = float(len_x * n_gx * len_y * n_gy)

    def control(total, step):
        means = total[0:4, 0:len_z] * (1.0 / cells_total)
        prof_ref[0:3, :] += means[0:3] * (1.0 / STEPS)
        prof_ref[3:4, :] += (means[3:4] - means[0:1] * means[2:3]) * (1.0 / STEPS)
        nudge = (target_ref[...] - means[0:2]) * (TIME_STEP / RELAX_TIME)
        for c in range(2):
            nudge_ref[c] = jnp.broadcast_to(nudge[c : c + 1], (8, len_z))

        @pl.when(step == 0)
        def _():
            area_ref[...] = total[5:6, 0:turbines]
            integral_ref[...] = total[6:7, 0:turbines]

        speed = total[4:5, 0:turbines] / area_ref[...]
        error = speed - rated
        integral = integral_ref[...] + CONTROL_STEP * error
        integral_ref[...] = integral
        thrust = 0.1 + 0.9 * jax.nn.sigmoid(
            bias - GAIN_PROPORTIONAL * error - GAIN_INTEGRAL * integral
        )
        thrust_ref[...] = thrust
        strength = (-0.5 * TIME_STEP) * thrust * speed * jnp.abs(speed)
        for s in range(slots):
            factor_ref[s] = jnp.sum(strength * hot(s))

    reset()
    load.wait()
    lax.fori_loop(0, len_x, first_plane, 0)

    def step_body(step, carry):
        parity = lax.rem(step, 2)
        total = reduce_all(parity)
        control(total, step)
        reset()
        for side in range(2):
            y_copy(parity, side, False).wait()
        for chunk in range(CHUNKS):
            for side in range(2):
                x_copy(parity, side, chunk, False).wait()
            lower = chunk * rows

            def edge(i, carry):
                sweep(parity, i + (i // 2) * (len_x - 4), lower, lower + rows)
                return carry

            lax.fori_loop(0, 4, edge, 0)

            @pl.when(step < STEPS - 1)
            def _():
                for side in range(2):
                    x_copy(1 - parity, side, chunk, False).start()

        def inner(x, carry):
            sweep(parity, x, 0, len_y)
            return carry

        lax.fori_loop(2, len_x - 2, inner, 0)

        @pl.when(step < STEPS - 1)
        def _():
            for side in range(2):
                y_copy(1 - parity, side, False).start()

        return carry

    lax.fori_loop(0, STEPS, step_body, 0)
    store = pltpu.make_async_copy(
        buf.at[STEPS % 2, :, pl.ds(2, len_x), pl.ds(PAD, len_y), :], out_ref, load_sem
    )
    store.start()
    lane_o = lax.broadcasted_iota(jnp.int32, (1, owned), 1)
    result = jnp.zeros((1, owned), jnp.float32)
    for r in range(owned):
        mine_r = mine_ref[r : r + 1, :]
        value = jnp.sum(mine_r * integral_ref[...]) + (1.0 - jnp.sum(mine_r)) * state_ref[0, r]
        result = jnp.where(lane_o == r, value, result)
    next_ref[...] = result
    store.wait()


def local(
    n_gx,
    n_gy,
    velocity,
    target_profile,
    disc_turbine,
    disc_start,
    disc_weight,
    turbine_owner,
    mode_flag,
    controller_state,
):
    _, len_x, len_y, len_z = velocity.shape
    turbines = mode_flag.shape[0]
    slots = disc_turbine.shape[1]
    owned = controller_state.shape[1]
    wide = -(-max(len_z, turbines) // 128) * 128
    any_spec = pl.BlockSpec(memory_space=pl.ANY)
    vmem = pl.BlockSpec(memory_space=pltpu.VMEM)
    smem = pl.BlockSpec(memory_space=pltpu.SMEM)
    f32 = jnp.float32
    dma = pltpu.SemaphoreType.DMA
    out, prof, thrust, following = pl.pallas_call(
        functools.partial(kernel, n_gx, n_gy),
        out_shape=(
            jax.ShapeDtypeStruct(velocity.shape, f32),
            jax.ShapeDtypeStruct((4, len_z), f32),
            jax.ShapeDtypeStruct((1, turbines), f32),
            jax.ShapeDtypeStruct((1, owned), f32),
        ),
        in_specs=[any_spec, vmem, smem, smem, vmem, vmem, vmem, smem],
        out_specs=(any_spec, vmem, vmem, vmem),
        scratch_shapes=[
            pltpu.VMEM((2, 3, len_x + 4, len_y + 2 * PAD, len_z), f32),
            pltpu.VMEM((slots, len_y, len_z), f32),
            pltpu.VMEM((4, 8, len_z), f32),
            pltpu.VMEM((slots, 8, 128), f32),
            pltpu.VMEM((2, 8, wide), f32),
            pltpu.VMEM((2, n_gy, 8, wide), f32),
            pltpu.VMEM((2, n_gx, 8, wide), f32),
            dma((2, CHUNKS)),
            dma((2, 2, CHUNKS)),
            dma((2,)),
            dma((2, 2)),
            dma,
            dma((n_gy,)),
            dma((2, n_gy)),
            dma((n_gx,)),
            dma((2, n_gx)),
            pltpu.VMEM((1, turbines), f32),
            pltpu.VMEM((1, turbines), f32),
            pltpu.SMEM((slots,), f32),
            pltpu.VMEM((owned, turbines), f32),
            pltpu.VMEM((2, 8, len_z), f32),
        ],
        compiler_params=pltpu.CompilerParams(
            collective_id=0, has_side_effects=True, vmem_limit_bytes=48 * 1024 * 1024
        ),
    )(
        velocity,
        target_profile,
        disc_turbine,
        disc_start,
        disc_weight,
        turbine_owner[None, :],
        mode_flag[None, :],
        controller_state,
    )
    return out, prof, thrust[0], following


def solution(mesh):
    placed = (
        P(None, "gx", "gy", None),
        P(),
        P(("gx", "gy"), None),
        P(None, ("gx", "gy"), None),
        P(("gx", "gy"), None, None, None),
        P(),
        P(),
        P(("gx", "gy"), None),
    )
    return jax.shard_map(
        functools.partial(local, mesh.shape["gx"], mesh.shape["gy"]),
        mesh=mesh,
        in_specs=placed,
        out_specs=(P(None, "gx", "gy", None), P(), P(), P(("gx", "gy"), None)),
        check_vma=False,
    )
```

```python
import functools

import jax
import jax.numpy as jnp
from jax import lax
from jax.experimental import pallas as pl
from jax.experimental.pallas import tpu as pltpu
from jax.sharding import PartitionSpec as P

STEPS = 4

VISCOSITY = 0.1
TIME_STEP = 0.2
RELAX_TIME = 2.0
CONTROL_STEP = 0.5
GAIN_PROPORTIONAL = 2.0
GAIN_INTEGRAL = 1.0
HIGHEST = lax.Precision.HIGHEST
MESH = pl.DeviceIdType.MESH
PAD = 8
CHUNKS = 4


def kernel(
    n_gx,
    n_gy,
    vel_ref,
    target_in,
    turbine_in,
    start_in,
    weight_in,
    owner_in,
    mode_in,
    state_in,
    out_ref,
    prof_ref,
    thrust_ref,
    next_ref,
    buf,
    dense,
    acc,
    acc_disc,
    pay,
    gather_y,
    gather_x,
    send_x,
    recv_x,
    send_y,
    recv_y,
    load_sem,
    send_1,
    recv_1,
    send_2,
    recv_2,
    integral_ref,
    area_ref,
    factor_ref,
    mine_ref,
    nudge_ref,
    target_ref,
    turbine_ref,
    start_ref,
    weight_ref,
    owner_ref,
    mode_ref,
    state_ref,
    small_sem,
    store_sem,
):
    len_x, len_y, len_z = vel_ref.shape[1:]
    slots, tile_y, tile_z = weight_in.shape[1:]
    owned = state_in.shape[1]
    turbines = owner_in.shape[1]
    gx = lax.axis_index("gx")
    gy = lax.axis_index("gy")
    right_x = (lax.rem(gx + 1, n_gx), gy)
    left_x = (lax.rem(gx + n_gx - 1, n_gx), gy)
    right_y = (gx, lax.rem(gy + 1, n_gy))
    left_y = (gx, lax.rem(gy + n_gy - 1, n_gy))
    rows = len_y // CHUNKS

    barrier = pltpu.get_barrier_semaphore()
    for d in range(1, n_gy):
        pl.semaphore_signal(barrier, inc=1, device_id=(gx, lax.rem(gy + d, n_gy)), device_id_type=MESH)
    for d in range(1, n_gx):
        pl.semaphore_signal(barrier, inc=1, device_id=(lax.rem(gx + d, n_gx), gy), device_id_type=MESH)

    load = pltpu.make_async_copy(
        vel_ref, buf.at[0, :, pl.ds(2, len_x), pl.ds(PAD, len_y), :], load_sem
    )
    small = [
        pltpu.make_async_copy(source, place, small_sem.at[i])
        for i, (source, place) in enumerate(
            [
                (weight_in, weight_ref),
                (start_in, start_ref),
                (turbine_in, turbine_ref),
                (owner_in, owner_ref),
                (mode_in, mode_ref),
                (state_in, state_ref),
                (target_in, target_ref),
            ]
        )
    ]
    for copy in small:
        copy.start()
    pl.semaphore_wait(barrier, n_gx + n_gy - 2)

    def x_copy(parity, side, chunk, first):
        at = PAD + chunk * rows
        begin = len_x - 2 if side == 0 else 0
        if first:
            source = vel_ref.at[:, pl.ds(begin, 2), pl.ds(chunk * rows, rows), :]
        else:
            source = buf.at[parity, :, pl.ds(begin + 2, 2), pl.ds(at, rows), :]
        place = 0 if side == 0 else len_x + 2
        return pltpu.make_async_remote_copy(
            src_ref=source,
            dst_ref=buf.at[parity, :, pl.ds(place, 2), pl.ds(at, rows), :],
            send_sem=send_x.at[side, chunk],
            recv_sem=recv_x.at[parity, side, chunk],
            device_id=right_x if side == 0 else left_x,
            device_id_type=MESH,
        )

    def y_copy(parity, side, first):
        begin = len_y - PAD if side == 0 else 0
        if first:
            source = vel_ref.at[:, :, pl.ds(begin, PAD), :]
        else:
            source = buf.at[parity, :, pl.ds(2, len_x), pl.ds(PAD + begin, PAD), :]
        place = 0 if side == 0 else PAD + len_y
        return pltpu.make_async_remote_copy(
            src_ref=source,
            dst_ref=buf.at[parity, :, pl.ds(2, len_x), pl.ds(place, PAD), :],
            send_sem=send_y.at[side],
            recv_sem=recv_y.at[parity, side],
            device_id=right_y if side == 0 else left_y,
            device_id_type=MESH,
        )

    for side in range(2):
        y_copy(0, side, True).start()
    for chunk in range(CHUNKS):
        for side in range(2):
            x_copy(0, side, chunk, True).start()
    load.start()
    for copy in small:
        copy.wait()

    for s in range(slots):
        rows_hot = (
            lax.broadcasted_iota(jnp.int32, (len_y, tile_y), 0)
            - lax.broadcasted_iota(jnp.int32, (len_y, tile_y), 1)
            == start_ref[1, 0, s]
        ).astype(jnp.float32)
        cols_hot = (
            lax.broadcasted_iota(jnp.int32, (tile_z, len_z), 1)
            - lax.broadcasted_iota(jnp.int32, (tile_z, len_z), 0)
            == start_ref[2, 0, s]
        ).astype(jnp.float32)
        tall = jnp.dot(rows_hot, weight_ref[0, s], precision=HIGHEST, preferred_element_type=jnp.float32)
        dense[s] = jnp.dot(tall, cols_hot, precision=HIGHEST, preferred_element_type=jnp.float32)

    lane_t = lax.broadcasted_iota(jnp.int32, (1, turbines), 1)

    def hot(s):
        return (lane_t == turbine_ref[0, s]).astype(jnp.float32)

    owner = owner_ref[...]
    me = gx * n_gy + gy
    pair_row = lax.broadcasted_iota(jnp.int32, (turbines, turbines), 0)
    pair_col = lax.broadcasted_iota(jnp.int32, (turbines, turbines), 1)
    owner_f = owner.astype(jnp.float32)
    owner_column = jnp.sum(jnp.where(pair_row == pair_col, owner_f, 0.0), axis=1, keepdims=True)
    rank = jnp.sum(
        jnp.where((owner_column == owner_f) & (pair_row < pair_col), 1.0, 0.0), axis=0, keepdims=True
    )
    is_me = jnp.where(owner == me, 1.0, 0.0)
    mine_integral = jnp.zeros((1, turbines), jnp.float32)
    area = jnp.zeros((1, turbines), jnp.float32)
    for r in range(owned):
        mine_r = jnp.where(rank == float(r), is_me, 0.0)
        mine_ref[r : r + 1, :] = mine_r
        mine_integral = mine_integral + mine_r * state_ref[0, r]
    for s in range(slots):
        area = area + jnp.sum(weight_ref[0, s]) * hot(s)
    pay[...] = jnp.zeros_like(pay)
    pay[0, 5:6, 0:turbines] = area
    pay[0, 6:7, 0:turbines] = mine_integral

    mode = mode_ref[...]
    rated = jnp.where(mode == 0, 0.7, jnp.where(mode == 1, 0.9, 1.1)).astype(jnp.float32)
    bias = jnp.where(mode == 0, 1.0, jnp.where(mode == 1, 0.0, -1.0)).astype(jnp.float32)
    prof_ref[...] = jnp.zeros_like(prof_ref)

    lane = lax.broadcasted_iota(jnp.int32, (8, len_z), 1)
    keep_m1 = lane >= 1
    keep_m2 = lane >= 2
    keep_p1 = lane < len_z - 1
    keep_p2 = lane < len_z - 2

    def fold(value):
        total = value[:, 0:128]
        for z in range(128, len_z, 128):
            total = total + value[:, z : z + 128]
        return total

    def tally(x, values):
        sums = None
        discs = [None] * slots
        for group, u, v, w in values:
            terms = [u, v, w, u * w]
            sums = terms if sums is None else [a + b for a, b in zip(sums, terms)]
            for s in range(slots):
                part = dense[s, group : group + 8, :] * u
                discs[s] = part if discs[s] is None else discs[s] + part
        for c in range(4):
            acc[c] += sums[c]
        for s in range(slots):
            here = jnp.where(start_ref[0, 0, s] == x, 1.0, 0.0)
            acc_disc[s] += fold(discs[s]) * here

    def reset():
        acc[...] = jnp.zeros_like(acc)
        acc_disc[...] = jnp.zeros_like(acc_disc)

    def first_plane(x, carry):
        tally(
            x,
            [
                (g, *[buf[0, c, x + 2, PAD + g : PAD + g + 8, :] for c in range(3)])
                for g in range(0, len_y, 8)
            ],
        )
        return carry

    def update(parity, x, group):
        at = PAD + group

        def cells(c, dx, dy):
            return buf[parity, c, x + 2 + dx, at + dy : at + dy + 8, :]

        centre = [cells(c, 0, 0) for c in range(3)]
        scaled = [f * (TIME_STEP / 12.0) for f in centre]
        fresh = []
        for c in range(3):
            f = centre[c]
            xp, xm = cells(c, 1, 0), cells(c, -1, 0)
            yp, ym = cells(c, 0, 1), cells(c, 0, -1)
            zp = jnp.where(keep_p1, pltpu.roll(f, len_z - 1, 1), 0.0)
            zm = jnp.where(keep_m1, pltpu.roll(f, 1, 1), 0.0)
            zp2 = jnp.where(keep_p2, pltpu.roll(f, len_z - 2, 1), 0.0)
            zm2 = jnp.where(keep_m2, pltpu.roll(f, 2, 1), 0.0)
            grad_x = 8.0 * (xp - xm) - (cells(c, 2, 0) - cells(c, -2, 0))
            grad_y = 8.0 * (yp - ym) - (cells(c, 0, 2) - cells(c, 0, -2))
            grad_z = 8.0 * (zp - zm) - (zp2 - zm2)
            around = (xp + xm) + (yp + ym) + (zp + zm)
            advection = scaled[0] * grad_x + scaled[1] * grad_y + scaled[2] * grad_z
            fresh.append(
                (1.0 - 6.0 * TIME_STEP * VISCOSITY) * f + (TIME_STEP * VISCOSITY) * around - advection
            )
        push = nudge_ref[0]
        for s in range(slots):
            gain = jnp.where(start_ref[0, 0, s] == x, factor_ref[s], 0.0)
            push = push + gain * dense[s, group : group + 8, :]
        fresh[0] = fresh[0] + push
        fresh[1] = fresh[1] + nudge_ref[1]
        for c in range(3):
            buf[1 - parity, c, x + 2, at : at + 8, :] = fresh[c]
        return (group, *fresh)

    def sweep(parity, x, lower, upper):
        tally(x, [update(parity, x, g) for g in range(lower, upper, 8)])

    def reduce_all(parity, step):
        numerator = jnp.zeros((1, turbines), jnp.float32)
        for s in range(slots):
            numerator = numerator + jnp.sum(acc_disc[s]) * hot(s)
        for c in range(4):
            pay[0, c : c + 1, 0:len_z] = jnp.sum(acc[c], axis=0, keepdims=True)
        pay[0, 4:5, 0:turbines] = numerator
        copies = []
        for d in range(1, n_gy):
            copies.append(
                pltpu.make_async_remote_copy(
                    src_ref=pay.at[0],
                    dst_ref=gather_y.at[parity, gy],
                    send_sem=send_1.at[d],
                    recv_sem=recv_1.at[parity, gy],
                    device_id=(gx, lax.rem(gy + d, n_gy)),
                    device_id_type=MESH,
                )
            )
            copies[-1].start()
        gather_y[parity, gy] = pay[0]
        for d in range(1, n_gy):
            sender = lax.rem(gy + d, n_gy)
            pltpu.make_async_remote_copy(
                src_ref=pay.at[0],
                dst_ref=gather_y.at[parity, sender],
                send_sem=send_1.at[d],
                recv_sem=recv_1.at[parity, sender],
                device_id=(gx, sender),
                device_id_type=MESH,
            ).wait_recv()
        total = gather_y[parity, 0]
        for d in range(1, n_gy):
            total = total + gather_y[parity, d]
        pay[1] = total
        for d in range(1, n_gx):
            copies.append(
                pltpu.make_async_remote_copy(
                    src_ref=pay.at[1],
                    dst_ref=gather_x.at[parity, gx],
                    send_sem=send_2.at[d],
                    recv_sem=recv_2.at[parity, gx],
                    device_id=(lax.rem(gx + d, n_gx), gy),
                    device_id_type=MESH,
                )
            )
            copies[-1].start()

        @pl.when(step > 0)
        def _():
            for side in range(2):
                x_copy(parity, side, CHUNKS - 1, False).start()

        gather_x[parity, gx] = total
        for d in range(1, n_gx):
            sender = lax.rem(gx + d, n_gx)
            pltpu.make_async_remote_copy(
                src_ref=pay.at[1],
                dst_ref=gather_x.at[parity, sender],
                send_sem=send_2.at[d],
                recv_sem=recv_2.at[parity, sender],
                device_id=(sender, gy),
                device_id_type=MESH,
            ).wait_recv()
        for copy in copies:
            copy.wait_send()
        total = gather_x[parity, 0]
        for d in range(1, n_gx):
            total = total + gather_x[parity, d]
        return total

    cells_total = float(len_x * n_gx * len_y * n_gy)

    def control(total, step):
        means = total[0:4, 0:len_z] * (1.0 / cells_total)
        prof_ref[0:3, :] += means[0:3] * (1.0 / STEPS)
        prof_ref[3:4, :] += (means[3:4] - means[0:1] * means[2:3]) * (1.0 / STEPS)
        nudge = (target_ref[...] - means[0:2]) * (TIME_STEP / RELAX_TIME)
        for c in range(2):
            nudge_ref[c] = jnp.broadcast_to(nudge[c : c + 1], (8, len_z))

        @pl.when(step == 0)
        def _():
            area_ref[...] = total[5:6, 0:turbines]
            integral_ref[...] = total[6:7, 0:turbines]

        speed = total[4:5, 0:turbines] / area_ref[...]
        error = speed - rated
        integral = integral_ref[...] + CONTROL_STEP * error
        integral_ref[...] = integral
        thrust = 0.1 + 0.9 * jax.nn.sigmoid(
            bias - GAIN_PROPORTIONAL * error - GAIN_INTEGRAL * integral
        )
        thrust_ref[...] = thrust
        strength = (-0.5 * TIME_STEP) * thrust * speed * jnp.abs(speed)
        for s in range(slots):
            factor_ref[s] = jnp.sum(strength * hot(s))

    reset()
    load.wait()
    lax.fori_loop(0, len_x, first_plane, 0)

    def store(part):
        begin, size = [(2, len_x - 4), (0, 2), (len_x - 2, 2)][part]
        return pltpu.make_async_copy(
            buf.at[STEPS % 2, :, pl.ds(2 + begin, size), pl.ds(PAD, len_y), :],
            out_ref.at[:, pl.ds(begin, size), :, :],
            store_sem.at[part],
        )

    def step_body(step, carry):
        parity = lax.rem(step, 2)
        total = reduce_all(parity, step)
        control(total, step)
        reset()
        for side in range(2):
            y_copy(parity, side, False).wait()
        def edges(chunk):
            for side in range(2):
                x_copy(parity, side, chunk, False).wait()
            lower = chunk * rows

            def edge(i, carry):
                sweep(parity, i + (i // 2) * (len_x - 4), lower, lower + rows)
                return carry

            lax.fori_loop(0, 4, edge, 0)

            @pl.when(step < STEPS - 1)
            def _():
                for side in range(2):
                    if chunk < CHUNKS - 1:
                        x_copy(1 - parity, side, chunk, False).start()

        def inner(x, carry):
            sweep(parity, x, 0, len_y)
            return carry

        for chunk in range(CHUNKS):
            edges(chunk)
            if chunk == CHUNKS - 2:
                lax.fori_loop(2, len_x - 2, inner, 0)

                @pl.when(step == STEPS - 1)
                def _():
                    store(0).start()

        @pl.when(step < STEPS - 1)
        def _():
            for side in range(2):
                y_copy(1 - parity, side, False).start()

        return carry

    lax.fori_loop(0, STEPS, step_body, 0)
    store(1).start()
    store(2).start()
    lane_o = lax.broadcasted_iota(jnp.int32, (1, owned), 1)
    result = jnp.zeros((1, owned), jnp.float32)
    for r in range(owned):
        mine_r = mine_ref[r : r + 1, :]
        value = jnp.sum(mine_r * integral_ref[...]) + (1.0 - jnp.sum(mine_r)) * state_ref[0, r]
        result = jnp.where(lane_o == r, value, result)
    next_ref[...] = result
    for part in range(3):
        store(part).wait()


def local(
    n_gx,
    n_gy,
    velocity,
    target_profile,
    disc_turbine,
    disc_start,
    disc_weight,
    turbine_owner,
    mode_flag,
    controller_state,
):
    _, len_x, len_y, len_z = velocity.shape
    turbines = mode_flag.shape[0]
    slots = disc_turbine.shape[1]
    owned = controller_state.shape[1]
    wide = -(-max(len_z, turbines) // 128) * 128
    any_spec = pl.BlockSpec(memory_space=pl.ANY)
    vmem = pl.BlockSpec(memory_space=pltpu.VMEM)
    hbm = pl.BlockSpec(memory_space=pltpu.HBM)
    f32 = jnp.float32
    dma = pltpu.SemaphoreType.DMA
    out, prof, thrust, following = pl.pallas_call(
        functools.partial(kernel, n_gx, n_gy),
        out_shape=(
            jax.ShapeDtypeStruct(velocity.shape, f32),
            jax.ShapeDtypeStruct((4, len_z), f32),
            jax.ShapeDtypeStruct((1, turbines), f32),
            jax.ShapeDtypeStruct((1, owned), f32),
        ),
        in_specs=[hbm] * 8,
        out_specs=(any_spec, vmem, vmem, vmem),
        scratch_shapes=[
            pltpu.VMEM((2, 3, len_x + 4, len_y + 2 * PAD, len_z), f32),
            pltpu.VMEM((slots, len_y, len_z), f32),
            pltpu.VMEM((4, 8, len_z), f32),
            pltpu.VMEM((slots, 8, 128), f32),
            pltpu.VMEM((2, 8, wide), f32),
            pltpu.VMEM((2, n_gy, 8, wide), f32),
            pltpu.VMEM((2, n_gx, 8, wide), f32),
            dma((2, CHUNKS)),
            dma((2, 2, CHUNKS)),
            dma((2,)),
            dma((2, 2)),
            dma,
            dma((n_gy,)),
            dma((2, n_gy)),
            dma((n_gx,)),
            dma((2, n_gx)),
            pltpu.VMEM((1, turbines), f32),
            pltpu.VMEM((1, turbines), f32),
            pltpu.SMEM((slots,), f32),
            pltpu.VMEM((owned, turbines), f32),
            pltpu.VMEM((2, 8, len_z), f32),
            pltpu.VMEM(target_profile.shape, f32),
            pltpu.SMEM(disc_turbine.shape, jnp.int32),
            pltpu.SMEM(disc_start.shape, jnp.int32),
            pltpu.VMEM(disc_weight.shape, f32),
            pltpu.VMEM((1, turbines), jnp.int32),
            pltpu.VMEM((1, turbines), jnp.int32),
            pltpu.SMEM(controller_state.shape, f32),
            dma((7,)),
            dma((3,)),
        ],
        compiler_params=pltpu.CompilerParams(
            collective_id=0, has_side_effects=True, vmem_limit_bytes=67_043_328
        ),
    )(
        velocity,
        target_profile,
        disc_turbine,
        disc_start,
        disc_weight,
        turbine_owner[None, :],
        mode_flag[None, :],
        controller_state,
    )
    return out, prof, thrust[0], following


def solution(mesh):
    placed = (
        P(None, "gx", "gy", None),
        P(),
        P(("gx", "gy"), None),
        P(None, ("gx", "gy"), None),
        P(("gx", "gy"), None, None, None),
        P(),
        P(),
        P(("gx", "gy"), None),
    )
    return jax.shard_map(
        functools.partial(local, mesh.shape["gx"], mesh.shape["gy"]),
        mesh=mesh,
        in_specs=placed,
        out_specs=(P(None, "gx", "gy", None), P(), P(), P(("gx", "gy"), None)),
        check_vma=False,
    )
```
